32 devices in a mesh: left: 8 (over y, x, core), right: 4 (over z).
Axes of the slice: x: 2, y: 2, z: 4, core: 2. Of those that a mesh axis runs over, the one named last changes fastest.
Arguments:
- signal: float32 [256, 256, 1024], P(None, 'left', 'right'), may hold values from -6 to 6
- symbol_x: float32 [256], replicated, may hold values from 0.3 to 3
- symbol_y: float32 [256], replicated, may hold values from 0.3 to 3
- symbol_z: float32 [1024], replicated, may hold values from 0.3 to 3
Outputs:
- spectrum: float32 [128, 128, 512], P('left', 'right')
The draws below stay inside these ranges and needn't reach their ends.
All inputs are finite; a program needn't handle non-finite values.
Results may differ from the reference program's by a relative error of at most 0.000096.
Values sent between devices are 32-bit elements; how exact they have to be, the bound alone decides.
No kernel may reach another device: no remote copies, remote signals or barrier semaphores. Data moves between devices by JAX's collectives and lax.ppermute only.
A program may use at most 128 MiB of HBM per device.

```python
import jax
import jax.numpy as jnp
from jax import lax

GRID_X = 256
GRID_Y = 256
GRID_Z = 1024


def steps_of(stream_key, extent, shards, smallest, largest):
    gain = 1.0
    for position, blocks in shards:
        steps = jax.random.uniform(jax.random.fold_in(jax.random.fold_in(stream_key, 6), position), (blocks,), jnp.float32, smallest / len(shards), largest / len(shards))
        gain = gain * jnp.repeat(jnp.exp(steps), extent[position] // blocks).reshape((-1,) + (1,) * (len(extent) - 1 - position))
    return gain


def normal_values(stream_key, extent, spread, most, split=(), dtype=jnp.bfloat16):
    level = steps_of(stream_key, extent, split, -0.22, 0.18) if split else 1.0
    result = jax.random.normal(stream_key, extent, jnp.float32) * spread * level
    return jnp.minimum(jnp.maximum(result, -most), most).astype(dtype)


def setup_inputs(seed: int = 0) -> dict:
    splits = jax.random.split(jax.random.key(seed), 5)
    return {
        "signal": normal_values(splits[0], (GRID_X, GRID_Y, GRID_Z), 1.0, 6.0, ((1, 8), (2, 4)), jnp.float32),
        "symbol_x": jnp.clip(jax.random.uniform(splits[1], (GRID_X,), jnp.float32, 0.3, 3.0), 0.3, 3.0),
        "symbol_y": jnp.clip(jax.random.uniform(splits[2], (GRID_Y,), jnp.float32, 0.3, 3.0), 0.3, 3.0),
        "symbol_z": jnp.clip(jax.random.uniform(splits[3], (GRID_Z,), jnp.float32, 0.3, 3.0), 0.3, 3.0),
    }


def transform_table(count):
    rank = jnp.arange(count)
    angle = (jnp.pi / (4 * count)) * (((2 * rank[:, None] + 1) * (2 * rank[None, :] + 1)) % (8 * count)).astype(jnp.float32)
    return jnp.cos(angle) * (2.0 / count) ** 0.5


def transform_dim(values, dim):
    moved = jnp.tensordot(values, transform_table(values.shape[dim]), axes=([dim], [0]), precision=lax.Precision.HIGHEST)
    return jnp.moveaxis(moved, -1, dim)


def reference(signal, symbol_x, symbol_y, symbol_z):
    spectrum = signal
    spectrum = transform_dim(spectrum, 0)
    spectrum = lax.slice_in_dim(spectrum, 0, GRID_X // 2, axis=0)
    spectrum = transform_dim(spectrum, 1)
    spectrum = lax.slice_in_dim(spectrum, 0, GRID_Y // 2, axis=1)
    spectrum = transform_dim(spectrum, 2)
    spectrum = lax.slice_in_dim(spectrum, 0, GRID_Z // 2, axis=2)
    symbol = symbol_x[:GRID_X // 2][:, None, None] + symbol_y[:GRID_Y // 2][None, :, None] + symbol_z[:GRID_Z // 2][None, None, :]
    spectrum = spectrum * ((1.0 - 0.2 * symbol) / (1.0 + 0.2 * symbol))
    return spectrum
```

```python
import jax
import jax.numpy as jnp
from jax import lax
from jax.experimental import pallas as pl
from jax.experimental.pallas import tpu as pltpu
from jax.sharding import PartitionSpec as P

LANES = 128
ROWS = 8
INTERPRET = False


def table_at(count, points, modes):
    angle = (
        jnp.pi
        / (4 * count)
        * ((2 * points[:, None] + 1) * (2 * modes[None, :] + 1) % (8 * count)).astype(jnp.float32)
    )
    return jnp.cos(angle) * (2.0 / count) ** 0.5


def split_table(table):
    high = lax.reduce_precision(table, 8, 7)
    return high.astype(jnp.bfloat16), (table - high).astype(jnp.bfloat16)


def split_values(values):
    high = values.astype(jnp.bfloat16)
    return high, (values - high.astype(jnp.float32)).astype(jnp.bfloat16)


def table_times(table_ref, values):
    modes = table_ref.shape[0] // 2
    high, low = split_values(values)
    both = jnp.dot(table_ref[...], high, preferred_element_type=jnp.float32)
    rest = jnp.dot(table_ref[:modes, :], low, preferred_element_type=jnp.float32)
    return both[:modes] + both[modes:] + rest


def call(kernel, **settings):
    return pl.pallas_call(kernel, interpret=INTERPRET, **settings)


def first_kernel(table_ref, signal_ref, *out_refs):
    count = signal_ref.shape[0]
    flat = signal_ref.reshape(count * ROWS, LANES)
    values = jnp.concatenate(
        [flat[pl.ds(row, count, stride=ROWS), :] for row in range(ROWS)], axis=1
    )
    moved = table_times(table_ref, values)
    share = out_refs[0].shape[1]
    for piece, out_ref in enumerate(out_refs):
        for row in range(ROWS):
            out_ref[row] = moved[
                piece * share : (piece + 1) * share, row * LANES : (row + 1) * LANES
            ]


def first_transform(table, signal, zone, pieces):
    count, lines, _ = signal.shape
    share = table.shape[0] // 2 // pieces
    return call(
        first_kernel,
        grid=(lines // ROWS,),
        in_specs=[
            pl.BlockSpec(table.shape, lambda step: (0, 0)),
            pl.BlockSpec((count, ROWS, LANES), lambda step: (0, step, zone)),
        ],
        out_specs=[pl.BlockSpec((ROWS, share, LANES), lambda step: (step, 0, 0))] * pieces,
        out_shape=[jax.ShapeDtypeStruct((lines, share, LANES), jnp.float32)] * pieces,
        name="first_transform",
    )(table, signal)


def second_kernel(table_ref, *refs, pieces_in):
    in_refs, out_refs = refs[:pieces_in], refs[pieces_in:]
    lines, share, _ = in_refs[0].shape
    flats = [in_ref.reshape(lines * share, LANES) for in_ref in in_refs]
    values = jnp.concatenate(
        [
            jnp.concatenate([flat[pl.ds(row, lines, stride=share), :] for flat in flats], axis=0)
            for row in range(share)
        ],
        axis=1,
    )
    moved = table_times(table_ref, values)
    modes = out_refs[0].shape[1]
    for piece, out_ref in enumerate(out_refs):
        for row in range(share):
            out_ref[row] = moved[
                piece * modes : (piece + 1) * modes, row * LANES : (row + 1) * LANES
            ]


def second_transform(table, arrived, pieces):
    share = arrived[0].shape[1]
    modes = table.shape[0] // 2 // pieces
    return call(
        lambda *refs: second_kernel(*refs, pieces_in=len(arrived)),
        out_shape=[jax.ShapeDtypeStruct((share, modes, LANES), jnp.float32)] * pieces,
        name="second_transform",
    )(table, *arrived)


def third_kernel(high_ref, low_ref, plane_ref, line_ref, *refs, pieces_in):
    in_refs, out_ref = refs[:pieces_in], refs[-1]
    share, modes, _ = in_refs[0].shape
    rows = share * modes
    values = jnp.concatenate(
        [in_ref[...].reshape(rows, LANES) for in_ref in in_refs], axis=1
    )
    high, low = split_values(values)
    moved = (
        jnp.dot(high, high_ref[...], preferred_element_type=jnp.float32)
        + jnp.dot(high, low_ref[...], preferred_element_type=jnp.float32)
        + jnp.dot(low, high_ref[...], preferred_element_type=jnp.float32)
    )
    symbol = plane_ref[...] + line_ref[...]
    moved = moved * ((1.0 - 0.2 * symbol) / (1.0 + 0.2 * symbol))
    out_ref[...] = moved.reshape(share, modes, moved.shape[1])


def third_transform(high, low, plane, line, arrived, before, block, blocks):
    share, modes, _ = arrived[0].shape
    rows = share * modes
    length = high.shape[1]
    whole = lambda array: pl.BlockSpec(array.shape, lambda step: (0,) * array.ndim)
    operands = [high, low, plane, line, *arrived]
    in_specs = [
        whole(high),
        whole(low),
        pl.BlockSpec((rows, 1), lambda step: (block, 0)),
        whole(line),
    ] + [whole(piece) for piece in arrived]
    aliases = {}
    if before is not None:
        aliases = {len(operands): 0}
        operands.append(before)
        in_specs.append(pl.BlockSpec(memory_space=pl.ANY))
    return call(
        lambda *refs: third_kernel(*refs, pieces_in=len(arrived)),
        grid=(1,),
        in_specs=in_specs,
        out_specs=pl.BlockSpec((share, modes, length), lambda step: (block, 0, 0)),
        out_shape=jax.ShapeDtypeStruct((share * blocks, modes, length), jnp.float32),
        input_output_aliases=aliases,
        name="third_transform",
    )(*operands)


def exchange(pieces, axis, members):
    return [pieces[0]] + [
        lax.ppermute(pieces[d], axis, [(source, source ^ d) for source in range(members)])
        for d in range(1, members)
    ]


def make_body(left, right):
    def body(signal, symbol_x, symbol_y, symbol_z):
        count_x, lines, depth = signal.shape
        count_y, count_z = lines * left, depth * right
        share_x, share_y = count_x // 2 // left, count_y // 2 // right
        blocks = share_x // ROWS
        zones = depth // LANES
        at_left, at_right = lax.axis_index("left"), lax.axis_index("right")
        left_peers = at_left ^ jnp.arange(left)
        right_peers = at_right ^ jnp.arange(right)

        modes_x = (
            left_peers[None, :, None] * share_x
            + (jnp.arange(blocks) * ROWS)[:, None, None]
            + jnp.arange(ROWS)[None, None, :]
        ).reshape(-1)
        points_y = (left_peers[:, None] * lines + jnp.arange(lines)[None, :]).reshape(-1)
        modes_y = (right_peers[:, None] * share_y + jnp.arange(share_y)[None, :]).reshape(-1)
        points_z = (
            right_peers[None, :, None] * depth
            + (jnp.arange(zones) * LANES)[:, None, None]
            + jnp.arange(LANES)[None, None, :]
        ).reshape(-1)

        table_x = jnp.concatenate(split_table(table_at(count_x, modes_x, jnp.arange(count_x))))
        table_y = jnp.concatenate(split_table(table_at(count_y, modes_y, points_y)))

        sent = [first_transform(table_x, signal, zone, blocks * left) for zone in range(zones)]
        arrived = {}
        for zone in range(zones):
            for block in range(blocks):
                pieces = sent[zone][block * left : (block + 1) * left]
                pieces = exchange(pieces, "left", left)
                pieces = second_transform(table_y, pieces, right)
                arrived[zone, block] = exchange(pieces, "right", right)

        high_z, low_z = split_table(table_at(count_z, points_z, jnp.arange(count_z // 2)))
        part_x = lax.dynamic_slice_in_dim(symbol_x, at_left * share_x, share_x)
        part_y = lax.dynamic_slice_in_dim(symbol_y, at_right * share_y, share_y)
        plane = (part_x[:, None] + part_y[None, :]).reshape(-1, 1)
        line = symbol_z[None, : count_z // 2]
        result = None
        for block in range(blocks):
            pieces = [piece for zone in range(zones) for piece in arrived[zone, block]]
            result = third_transform(high_z, low_z, plane, line, pieces, result, block, blocks)
        return result

    return body


def solution(mesh):
    in_specs = (P(None, "left", "right"), P(), P(), P())
    out_specs = P("left", "right", None)
    body = make_body(mesh.shape["left"], mesh.shape["right"])
    return jax.shard_map(body, mesh=mesh, in_specs=in_specs, out_specs=out_specs, check_vma=False)
```

```python
import jax
import jax.numpy as jnp
from jax import lax
from jax.experimental import pallas as pl
from jax.experimental.pallas import tpu as pltpu
from jax.sharding import PartitionSpec as P

LANES = 128
ROWS = 8
INTERPRET = False

AHEAD = 2
BLOCKS = 1
FINE = 32
LEFT_PERMUTES = True
RIGHT_PERMUTES = True


def table_at(count, points, modes):
    angle = (
        jnp.pi
        / (4 * count)
        * ((2 * points[:, None] + 1) * (2 * modes[None, :] + 1) % (8 * count)).astype(jnp.float32)
    )
    return jnp.cos(angle) * (2.0 / count) ** 0.5


def long_table(count, points, modes):
    odd = (2 * modes + 1)[None, :]
    scale = jnp.pi / (4 * count)
    coarse = scale * (2 * points[:, :1] * odd % (8 * count)).astype(jnp.float32)
    offsets = jnp.arange(points.shape[1])[:, None]
    fine = scale * ((2 * offsets + 1) * odd % (8 * count)).astype(jnp.float32)
    size = (2.0 / count) ** 0.5
    table = (
        jnp.cos(coarse)[:, None, :] * (jnp.cos(fine) * size)[None, :, :]
        - jnp.sin(coarse)[:, None, :] * (jnp.sin(fine) * size)[None, :, :]
    )
    return table.reshape(points.size, -1)


def split_table(table):
    high = lax.reduce_precision(table, 8, 7)
    return high.astype(jnp.bfloat16), (table - high).astype(jnp.bfloat16)


def split_values(values):
    high = values.astype(jnp.bfloat16)
    return high, (values - high.astype(jnp.float32)).astype(jnp.bfloat16)


def table_times(table_ref, values):
    modes = table_ref.shape[0] // 2
    high, low = split_values(values)
    both = jnp.dot(table_ref[...], high, preferred_element_type=jnp.float32)
    rest = jnp.dot(table_ref[:modes, :], low, preferred_element_type=jnp.float32)
    return both[:modes] + both[modes:] + rest


def call(kernel, **settings):
    return pl.pallas_call(kernel, interpret=INTERPRET, **settings)


def first_kernel(table_ref, signal_ref, *out_refs, blocks):
    count = signal_ref.shape[0]
    flat = signal_ref.reshape(count * ROWS, LANES)
    values = jnp.concatenate(
        [flat[pl.ds(row, count, stride=ROWS), :] for row in range(ROWS)], axis=1
    )
    moved = table_times(table_ref, values)
    peers, _, share, _ = out_refs[0].shape
    for index, out_ref in enumerate(out_refs):
        block, group = divmod(index, len(out_refs) // blocks)
        for peer in range(peers):
            start = ((group * peers + peer) * blocks + block) * share
            for row in range(ROWS):
                out_ref[peer, row] = moved[
                    start : start + share, row * LANES : (row + 1) * LANES
                ]


def first_transform(table, signal, zone, groups, blocks, share):
    count, lines, _ = signal.shape
    peers = table.shape[0] // 2 // groups // blocks // share
    arrays = groups * blocks
    out = call(
        lambda *refs: first_kernel(*refs, blocks=blocks),
        grid=(lines // ROWS,),
        in_specs=[
            pl.BlockSpec(table.shape, lambda step: (0, 0)),
            pl.BlockSpec((count, ROWS, LANES), lambda step: (0, step, zone)),
        ],
        out_specs=[pl.BlockSpec((peers, ROWS, share, LANES), lambda step: (0, step, 0, 0))] * arrays,
        out_shape=[jax.ShapeDtypeStruct((peers, lines, share, LANES), jnp.float32)] * arrays,
        name="first_transform",
    )(table, signal)
    return [out[block * groups : (block + 1) * groups] for block in range(blocks)]


def second_kernel(table_ref, *refs, pieces_in):
    in_refs, out_refs = refs[:pieces_in], refs[pieces_in:]
    peers, lines, share, _ = in_refs[0].shape
    flats = [in_ref.reshape(peers * lines * share, LANES) for in_ref in in_refs]
    values = jnp.concatenate(
        [
            jnp.concatenate(
                [flat[pl.ds(row, peers * lines, stride=share), :] for flat in flats], axis=0
            )
            for row in range(share)
        ],
        axis=1,
    )
    moved = table_times(table_ref, values)
    targets, _, modes, _ = out_refs[0].shape
    for group, out_ref in enumerate(out_refs):
        for peer in range(targets):
            start = (group * targets + peer) * modes
            for row in range(share):
                out_ref[peer, row] = moved[
                    start : start + modes, row * LANES : (row + 1) * LANES
                ]


def second_transform(table, arrived, peers, groups):
    share = arrived[0].shape[2]
    modes = table.shape[0] // 2 // peers
    return call(
        lambda *refs: second_kernel(*refs, pieces_in=len(arrived)),
        out_shape=[jax.ShapeDtypeStruct((peers // groups, share, modes, LANES), jnp.float32)] * groups,
        name="second_transform",
    )(table, *arrived)


def third_kernel(high_ref, low_ref, plane_ref, line_ref, *refs, pieces_in):
    in_refs, out_ref = refs[:pieces_in], refs[-1]
    peers, share, modes, _ = in_refs[0].shape
    rows = share * modes
    values = jnp.concatenate(
        [in_ref[peer].reshape(rows, LANES) for in_ref in in_refs for peer in range(peers)], axis=1
    )
    high, low = split_values(values)
    moved = (
        jnp.dot(high, high_ref[...], preferred_element_type=jnp.float32)
        + jnp.dot(high, low_ref[...], preferred_element_type=jnp.float32)
        + jnp.dot(low, high_ref[...], preferred_element_type=jnp.float32)
    )
    symbol = plane_ref[...] + line_ref[...]
    moved = moved * ((1.0 - 0.2 * symbol) / (1.0 + 0.2 * symbol))
    out_ref[...] = moved.reshape(share, modes, moved.shape[1])


def third_transform(high, low, plane, line, arrived, before, block, blocks):
    _, share, modes, _ = arrived[0].shape
    rows = share * modes
    length = high.shape[1]
    whole = lambda array: pl.BlockSpec(array.shape, lambda step: (0,) * array.ndim)
    operands = [high, low, plane, line, *arrived]
    in_specs = [
        whole(high),
        whole(low),
        pl.BlockSpec((rows, 1), lambda step: (block, 0)),
        whole(line),
    ] + [whole(piece) for piece in arrived]
    aliases = {}
    if before is not None:
        aliases = {len(operands): 0}
        operands.append(before)
        in_specs.append(pl.BlockSpec(memory_space=pl.ANY))
    return call(
        lambda *refs: third_kernel(*refs, pieces_in=len(arrived)),
        grid=(1,),
        in_specs=in_specs,
        out_specs=pl.BlockSpec((share, modes, length), lambda step: (block, 0, 0)),
        out_shape=jax.ShapeDtypeStruct((share * blocks, modes, length), jnp.float32),
        input_output_aliases=aliases,
        name="third_transform",
    )(*operands)


def exchange(pieces, axis, members):
    if len(pieces) == 1:
        return [lax.all_to_all(pieces[0], axis, split_axis=0, concat_axis=0, tiled=True)]
    return [pieces[0]] + [
        lax.ppermute(pieces[d], axis, [(source, source ^ d) for source in range(members)])
        for d in range(1, members)
    ]


def make_body(left, right):
    def body(signal, symbol_x, symbol_y, symbol_z):
        count_x, lines, depth = signal.shape
        count_y, count_z = lines * left, depth * right
        share_x, share_y = count_x // 2 // left, count_y // 2 // right
        blocks = BLOCKS
        share = share_x // blocks
        zones = depth // LANES
        at_left, at_right = lax.axis_index("left"), lax.axis_index("right")
        left_groups = left if LEFT_PERMUTES else 1
        right_groups = right if RIGHT_PERMUTES else 1
        left_peers = at_left ^ jnp.arange(left) if LEFT_PERMUTES else jnp.arange(left)
        right_peers = at_right ^ jnp.arange(right) if RIGHT_PERMUTES else jnp.arange(right)

        modes_x = (left_peers[:, None] * share_x + jnp.arange(share_x)[None, :]).reshape(-1)
        points_y = (left_peers[:, None] * lines + jnp.arange(lines)[None, :]).reshape(-1)
        modes_y = (right_peers[:, None] * share_y + jnp.arange(share_y)[None, :]).reshape(-1)
        starts_z = right_peers[None, :] * depth + (jnp.arange(zones) * LANES)[:, None]
        points_z = (
            starts_z[:, :, None, None]
            + (jnp.arange(LANES // FINE) * FINE)[None, None, :, None]
            + jnp.arange(FINE)
        ).reshape(-1, FINE)
        table_x = jnp.concatenate(split_table(table_at(count_x, modes_x, jnp.arange(count_x))))
        table_y = jnp.concatenate(split_table(table_at(count_y, modes_y, points_y)))

        chunks = [(zone, block) for zone in range(zones) for block in range(blocks)]
        sent = []
        for zone in range(zones):
            sent += first_transform(table_x, signal, zone, left_groups, blocks, share)
        received, moved = {}, {}
        for index, chunk in enumerate(chunks):
            pieces = sent[index]
            if index >= AHEAD:
                pieces, moved[index - AHEAD] = lax.optimization_barrier(
                    (pieces, moved[index - AHEAD])
                )
            pieces = exchange(pieces, "left", left)
            moved[index] = second_transform(table_y, pieces, right, right_groups)
        for index, chunk in enumerate(chunks):
            received[chunk] = exchange(moved[index], "right", right)

        high_z, low_z = split_table(long_table(count_z, points_z, jnp.arange(count_z // 2)))
        part_x = lax.dynamic_slice_in_dim(symbol_x, at_left * share_x, share_x)
        part_y = lax.dynamic_slice_in_dim(symbol_y, at_right * share_y, share_y)
        plane = (part_x[:, None] + part_y[None, :]).reshape(-1, 1)
        line = symbol_z[None, : count_z // 2]
        result = None
        for block in range(blocks):
            pieces = [piece for zone in range(zones) for piece in received[zone, block]]
            result = third_transform(high_z, low_z, plane, line, pieces, result, block, blocks)
        return result

    return body


def solution(mesh):
    in_specs = (P(None, "left", "right"), P(), P(), P())
    out_specs = P("left", "right", None)
    body = make_body(mesh.shape["left"], mesh.shape["right"])
    return jax.shard_map(body, mesh=mesh, in_specs=in_specs, out_specs=out_specs, check_vma=False)
```
